128 devices in a mesh: cand: 8 (over y, core), feat: 16 (over x, z).
Axes of the slice: x: 4, y: 4, z: 4, core: 2. Of those that a mesh axis runs over, the one named last changes fastest.
Arguments:
- embeddings: bfloat16 [262144, 4096], P('cand', 'feat'), may hold values from -1 to 1
- winners: int32 [3], replicated, may hold values from 0 to 262143, as said below
Outputs:
- gains: float32 [262144], P('cand')
- coords: float32 [3, 262144], P(None, 'cand')
- best: float32 [3], replicated
The draws below stay inside these ranges and needn't reach their ends.
Inputs may be any that keep to these rules, and one draw needn't show every extreme that they name: `winners`: 3 different candidates.
All inputs are finite; a program needn't handle non-finite values.
Results may differ from the reference program's by a relative error of at most 0.0003.
Values may be sent and summed in bfloat16 or wider, within the bound.
A program may use at most 128 MiB of HBM per device.

```python
import math
import jax
import jax.numpy as jnp
from jax import lax

D = 4096
STEPS = 3
CANDS = 262144


def draw_embeddings(key, part):
    keys = jax.random.split(jax.random.fold_in(key, 11), 5)
    noise = jnp.clip(jax.random.normal(keys[0], (CANDS, D), jnp.float32), -4.0, 4.0)
    shared = jax.random.uniform(keys[2], (CANDS, 1), jnp.float32, -1.0, 1.0)
    common = jnp.clip(jax.random.normal(keys[1], (1, D), jnp.float32), -4.0, 4.0)
    scales = jnp.exp(jax.random.uniform(keys[3], (CANDS, 1), jnp.float32, math.log(0.5), math.log(3.0)))
    rising = jnp.exp(math.log(3.0) * jnp.arange(D, dtype=jnp.float32) / D)[None, :]
    columns = rising * jax.random.uniform(keys[4], (1, D), jnp.float32, 0.7, 1.4)
    values = scales * columns * (noise + shared * common) / (1.8 * math.sqrt(D))
    return jnp.clip(values, -1.0, 1.0).astype(jnp.bfloat16)


def draw_winners(key, part):
    keys = jax.random.split(jax.random.fold_in(key, 23), 2)
    middle = jax.random.permutation(keys[0], CANDS - 2)[:STEPS - 2].astype(jnp.int32) + 1
    ends = jnp.array([0, CANDS - 1], dtype=jnp.int32)
    values = jnp.concatenate([ends, middle])
    order = jax.random.permutation(keys[1], STEPS)
    return values[order].astype(jnp.int32)


def setup_inputs(seed: int = 0) -> dict:
    streams_of = jax.random.split(jax.random.key(seed), 3)
    return {
        "embeddings": draw_embeddings(jax.random.fold_in(streams_of[2], 71), 0),
        "winners": draw_winners(jax.random.fold_in(streams_of[2], 71), 0),
    }


def reference(embeddings, winners):
    block = math.gcd(CANDS, 8192)
    blocks = embeddings.reshape(CANDS // block, block, D)
    norms = lax.map(lambda piece: lax.optimization_barrier(jnp.sum(jnp.square(piece.astype(jnp.float32)), axis=1)), blocks).reshape(CANDS)
    gains = norms
    coords = []
    best = []
    for step in range(STEPS):
        chosen = winners[step]
        row = lax.dynamic_index_in_dim(embeddings, chosen, 0, keepdims=False)
        dots = lax.map(lambda piece: jnp.dot(piece, row, preferred_element_type=jnp.float32), blocks).reshape(CANDS)
        proj = jnp.zeros((CANDS,), jnp.float32)
        for prior in range(step):
            proj = proj + coords[prior] * coords[prior][chosen]
        scale = jnp.sqrt(jnp.maximum(gains[chosen], 1.0))
        fresh = (dots - proj) / scale
        gains = gains - fresh * fresh
        coords.append(fresh)
        best.append(jnp.max(gains))
    return (gains, jnp.stack(coords), jnp.stack(best))
```

```python
import jax
import jax.numpy as jnp
from jax import lax
from jax.experimental import pallas as pl
from jax.experimental.pallas import tpu as pltpu
from jax.sharding import PartitionSpec as P

MESH = pl.DeviceIdType.MESH
STEPS = 3
CAND = 8
SIDE = 4
FEAT = SIDE * SIDE
ROWS = 32768
WIDTH = 256
HALF = ROWS // 2
QUART = HALF // SIDE
PIECE = QUART // SIDE
CHUNKS = 16
CHUNK = ROWS // CHUNKS
TILE = 512


def nt_dot(a, b):
    return lax.dot_general(a, b, (((1,), (1,)), ((), ())), preferred_element_type=jnp.float32)


def pick_kernel(win_ref, emb_ref, out_ref, blocks, sems):
    here = lax.axis_index("cand")
    copies = []
    for k in range(STEPS):
        row = lax.rem(win_ref[k], ROWS)
        start = pl.multiple_of(lax.div(row, 16) * 16, 16)
        copy = pltpu.make_async_copy(emb_ref.at[pl.ds(start, 16), :], blocks.at[k], sems.at[k])
        copy.start()
        copies.append(copy)
    out_ref[...] = jnp.zeros_like(out_ref)
    lines = lax.broadcasted_iota(jnp.int32, (16, WIDTH), 0)
    for k in range(STEPS):
        copies[k].wait()
        owner = lax.div(win_ref[k], ROWS)
        line = jnp.where(owner == here, lax.rem(win_ref[k], 16), -1)
        block = blocks[k].astype(jnp.float32)
        kept = jnp.where(lines == line, block, 0.0)
        out_ref[k : k + 1, :] = jnp.sum(kept, axis=0, keepdims=True)


def main_kernel(
    rows_ref, emb_ref, out_ref, best_ref,
    emb, part, won, gram_own, grams, in_a, in_b, sum_a, sum_b, in_c, in_d, whole, top, tops_c, tops_f,
    emb_sem, won_s, won_r, gram_s, gram_r, a_s, a_r, b_s, b_r, c_s, c_r, d_s, d_r,
    e_s, e_r, f_s, f_r, g_s, g_r, h_s, h_r, tc_s, tc_r, tf_s, tf_r, out_sem,
):
    c = lax.axis_index("cand")
    f = lax.axis_index("feat")
    x = lax.div(f, SIDE)
    z = lax.rem(f, SIDE)

    def load(i):
        lines = pl.ds(pl.multiple_of(i * CHUNK, CHUNK), CHUNK)
        return pltpu.make_async_copy(emb_ref.at[lines, :], emb.at[lines, :], emb_sem.at[i])

    for i in range(CHUNKS):
        load(i).start()

    def cand_peer(k):
        return (lax.rem(c + k, CAND), f)

    def x_peer(k):
        return (c, lax.rem(x + k, SIDE) * SIDE + z)

    def z_peer(k):
        return (c, x * SIDE + lax.rem(z + k, SIDE))

    def feat_peer(k):
        return (c, lax.rem(f + k, FEAT))

    def send(src, dst, s, r, k, peer):
        return pltpu.make_async_remote_copy(
            src_ref=src, dst_ref=dst, send_sem=s.at[k - 1], recv_sem=r.at[k - 1],
            device_id=peer, device_id_type=MESH,
        )

    barrier = pltpu.get_barrier_semaphore()
    for k in range(1, CAND):
        pl.semaphore_signal(barrier, inc=1, device_id=cand_peer(k), device_id_type=MESH)
    for k in range(1, FEAT):
        pl.semaphore_signal(barrier, inc=1, device_id=feat_peer(k), device_id_type=MESH)
    pl.semaphore_wait(barrier, CAND - 1 + FEAT - 1)

    won_out = [send(rows_ref, won.at[k - 1], won_s, won_r, k, cand_peer(k)) for k in range(1, CAND)]
    for copy in won_out:
        copy.start()

    ones = jnp.where(lax.broadcasted_iota(jnp.int32, (8, WIDTH), 0) == 3, 1.0, 0.0).astype(jnp.bfloat16)

    def norm_chunk(i, _):
        load(i).wait()

        def norm_tile(j, _):
            at = pl.multiple_of(i * CHUNK + j * TILE, TILE)
            e = emb[pl.ds(at, TILE), :].astype(jnp.float32)
            sq = e * e
            s = sq[:, :128] + sq[:, 128:]
            high = s.astype(jnp.bfloat16)
            low = (s - high.astype(jnp.float32)).astype(jnp.bfloat16)
            line = nt_dot(ones, jnp.concatenate([high, low], axis=1))
            part[:, pl.ds(at, TILE)] = line[0:4, :]
            return 0

        return lax.fori_loop(0, CHUNK // TILE, norm_tile, 0)

    lax.fori_loop(0, CHUNKS, norm_chunk, 0)

    for copy in won_out:
        copy.wait()
    total = rows_ref[...]
    for k in range(CAND - 1):
        total = total + won[k]
    w = total.astype(jnp.bfloat16)

    gram_own[...] = nt_dot(w, jnp.concatenate([w] * 16, axis=0))
    gram_out = [send(gram_own, grams.at[k - 1], gram_s, gram_r, k, feat_peer(k)) for k in range(1, FEAT)]
    for copy in gram_out:
        copy.start()

    def dots(base):
        def dot_tile(j, _):
            at = pl.multiple_of(base + j * TILE, TILE)
            line = nt_dot(w, emb[pl.ds(at, TILE), :])
            part[0:3, pl.ds(at, TILE)] = line[0:3, :]
            return 0

        lax.fori_loop(0, QUART // TILE, dot_tile, 0)

    def a_cols(xi):
        return pl.multiple_of(xi * QUART, QUART)

    def b_cols(zi):
        return pl.multiple_of(HALF + zi * QUART, QUART)

    first = []
    for k in (2, 1, 3, 0):
        at = a_cols(lax.rem(x + k, SIDE))
        dots(at)
        if k:
            copy = send(part.at[:, pl.ds(at, QUART)], in_a.at[k - 1], a_s, a_r, k, x_peer(k))
            copy.start()
            first.append(copy)
        at = b_cols(lax.rem(z + k, SIDE))
        dots(at)
        if k:
            copy = send(part.at[:, pl.ds(at, QUART)], in_b.at[k - 1], b_s, b_r, k, z_peer(k))
            copy.start()
            first.append(copy)
    for copy in first:
        copy.wait()

    second = []
    for k in (2, 1, 3, 0):
        zi = lax.rem(z + k, SIDE)
        here = pl.ds(pl.multiple_of(zi * PIECE, PIECE), PIECE)
        own = pl.ds(pl.multiple_of(a_cols(x) + zi * PIECE, PIECE), PIECE)
        sum_a[:, here] = part[:, own] + in_a[0, :, here] + in_a[1, :, here] + in_a[2, :, here]
        if k:
            copy = send(sum_a.at[:, here], in_c.at[k - 1], c_s, c_r, k, z_peer(k))
            copy.start()
            second.append(copy)
        xi = lax.rem(x + k, SIDE)
        here = pl.ds(pl.multiple_of(xi * PIECE, PIECE), PIECE)
        own = pl.ds(pl.multiple_of(b_cols(z) + xi * PIECE, PIECE), PIECE)
        sum_b[:, here] = part[:, own] + in_b[0, :, here] + in_b[1, :, here] + in_b[2, :, here]
        if k:
            copy = send(sum_b.at[:, here], in_d.at[k - 1], d_s, d_r, k, x_peer(k))
            copy.start()
            second.append(copy)

    for copy in gram_out:
        copy.wait()
    gram = gram_own[...]
    for k in range(FEAT - 1):
        gram = gram + grams[k]
    own_gain = [gram[s : s + 1, s : s + 1] for s in range(STEPS)]
    own_coord = [[None] * STEPS for _ in range(STEPS)]
    inverse = []
    for s in range(STEPS):
        inverse.append(1.0 / jnp.sqrt(jnp.maximum(own_gain[s], 1.0)))
        for later in range(s + 1, STEPS):
            value = gram[later : later + 1, s : s + 1]
            for prior in range(s):
                value = value - own_coord[later][prior] * own_coord[s][prior]
            value = value * inverse[s]
            own_coord[later][s] = value
            own_gain[later] = own_gain[later] - value * value

    for copy in second:
        copy.wait()

    def finish(sums, base, arrived, out_at):
        here = pl.ds(base, PIECE)
        t = sums[:, here] + arrived[0] + arrived[1] + arrived[2]
        gains = t[3:4, :]
        coords = []
        bests = []
        for s in range(STEPS):
            proj = t[s : s + 1, :]
            if s:
                back = jnp.zeros_like(proj)
                for prior in range(s):
                    back = back + coords[prior] * own_coord[s][prior]
                proj = proj - back
            fresh = proj * inverse[s]
            gains = gains - fresh * fresh
            coords.append(fresh)
            bests.append(jnp.max(gains, axis=1, keepdims=True))
            whole[s : s + 1, pl.ds(out_at, PIECE)] = fresh
        whole[3:4, pl.ds(out_at, PIECE)] = gains
        return bests

    own_a = pl.multiple_of(a_cols(x) + z * PIECE, PIECE)
    own_b = pl.multiple_of(b_cols(z) + x * PIECE, PIECE)
    best_a = finish(sum_a, pl.multiple_of(z * PIECE, PIECE), in_c, own_a)
    best_b = finish(sum_b, pl.multiple_of(x * PIECE, PIECE), in_d, own_b)
    lines = lax.broadcasted_iota(jnp.int32, (8, 128), 0)
    mine = jnp.zeros((8, 128), jnp.float32)
    for s in range(STEPS):
        mine = jnp.where(lines == s, jnp.maximum(best_a[s], best_b[s]), mine)
    top[0] = mine
    top_out = [send(top.at[0], tops_c.at[k - 1], tc_s, tc_r, k, cand_peer(k)) for k in range(1, CAND)]
    for copy in top_out:
        copy.start()

    third = []
    for k in (2, 1, 3):
        here = pl.ds(own_a, PIECE)
        copy = send(whole.at[:, here], whole.at[:, here], e_s, e_r, k, z_peer(k))
        copy.start()
        third.append(copy)
        here = pl.ds(own_b, PIECE)
        copy = send(whole.at[:, here], whole.at[:, here], f_s, f_r, k, x_peer(k))
        copy.start()
        third.append(copy)

    for copy in top_out:
        copy.wait()
    for k in range(CAND - 1):
        mine = jnp.maximum(mine, tops_c[k])
    top[1] = mine
    top_out = [send(top.at[1], tops_f.at[k - 1], tf_s, tf_r, k, feat_peer(k)) for k in range(1, FEAT)]
    for copy in top_out:
        copy.start()

    for copy in third:
        copy.wait()
    fourth = []
    for k in (2, 1, 3):
        here = pl.ds(a_cols(x), QUART)
        copy = send(whole.at[:, here], whole.at[:, here], g_s, g_r, k, x_peer(k))
        copy.start()
        fourth.append(copy)
        here = pl.ds(b_cols(z), QUART)
        copy = send(whole.at[:, here], whole.at[:, here], h_s, h_r, k, z_peer(k))
        copy.start()
        fourth.append(copy)
    for copy in top_out:
        copy.wait()
    for k in range(FEAT - 1):
        mine = jnp.maximum(mine, tops_f[k])
    best_ref[...] = mine
    for copy in fourth:
        copy.wait()
    done = pltpu.make_async_copy(whole, out_ref, out_sem)
    done.start()
    done.wait()


def per_device(embeddings, winners):
    rows = pl.pallas_call(
        pick_kernel,
        out_shape=jax.ShapeDtypeStruct((8, WIDTH), jnp.float32),
        in_specs=[pl.BlockSpec(memory_space=pltpu.SMEM), pl.BlockSpec(memory_space=pl.ANY)],
        out_specs=pl.BlockSpec(memory_space=pltpu.VMEM),
        scratch_shapes=[pltpu.VMEM((STEPS, 16, WIDTH), jnp.bfloat16), pltpu.SemaphoreType.DMA((STEPS,))],
        name="pick",
    )(winners, embeddings)
    f32 = jnp.float32
    sem = pltpu.SemaphoreType.DMA
    ring = [sem((SIDE - 1,)), sem((SIDE - 1,))]
    out, best = pl.pallas_call(
        main_kernel,
        out_shape=(jax.ShapeDtypeStruct((4, ROWS), f32), jax.ShapeDtypeStruct((8, 128), f32)),
        in_specs=[pl.BlockSpec(memory_space=pltpu.VMEM), pl.BlockSpec(memory_space=pl.ANY)],
        out_specs=(pl.BlockSpec(memory_space=pl.ANY), pl.BlockSpec(memory_space=pltpu.VMEM)),
        scratch_shapes=[
            pltpu.VMEM((ROWS, WIDTH), jnp.bfloat16),
            pltpu.VMEM((4, ROWS), f32),
            pltpu.VMEM((CAND - 1, 8, WIDTH), f32),
            pltpu.VMEM((8, 128), f32),
            pltpu.VMEM((FEAT - 1, 8, 128), f32),
            pltpu.VMEM((SIDE - 1, 4, QUART), f32),
            pltpu.VMEM((SIDE - 1, 4, QUART), f32),
            pltpu.VMEM((4, QUART), f32),
            pltpu.VMEM((4, QUART), f32),
            pltpu.VMEM((SIDE - 1, 4, PIECE), f32),
            pltpu.VMEM((SIDE - 1, 4, PIECE), f32),
            pltpu.VMEM((4, ROWS), f32),
            pltpu.VMEM((2, 8, 128), f32),
            pltpu.VMEM((CAND - 1, 8, 128), f32),
            pltpu.VMEM((FEAT - 1, 8, 128), f32),
            sem((CHUNKS,)),
            sem((CAND - 1,)), sem((CAND - 1,)),
            sem((FEAT - 1,)), sem((FEAT - 1,)),
            *ring, *ring, *ring, *ring, *ring, *ring, *ring, *ring,
            sem((CAND - 1,)), sem((CAND - 1,)),
            sem((FEAT - 1,)), sem((FEAT - 1,)),
            sem,
        ],
        compiler_params=pltpu.CompilerParams(
            collective_id=0, has_side_effects=True, vmem_limit_bytes=40 * 1024 * 1024
        ),
        name="main",
    )(rows, embeddings)
    return (out[3], out[:3], best[:STEPS, 0])


def solution(mesh):
    return jax.shard_map(
        per_device,
        mesh=mesh,
        in_specs=(P("cand", "feat"), P()),
        out_specs=(P("cand"), P(None, "cand"), P()),
        check_vma=False,
    )
```
